128 devices in a mesh: dp: 4 (over x), fsdp: 32 (over z, y, core).
Axes of the slice: x: 4, y: 4, z: 4, core: 2. Of those that a mesh axis runs over, the one named last changes fastest.
Arguments:
- gradient: bfloat16 [4, 4096, 8, 1024], P('dp', 'fsdp'), may hold values from -3 to 3
- block_owner_index: int32 [32], replicated, may hold values from 0 to 31, as said below
- block_grid_cell: int32 [32], replicated, may hold values from 0 to 31, each once
- left_eigen_basis: float32 [64, 1024, 1024], P('fsdp', None, 'dp'), may hold values from -0.1875 to 0.1875
- right_eigen_basis: float32 [64, 1024, 1024], P('fsdp', None, 'dp'), may hold values from -0.1875 to 0.1875
- left_statistic_matrix: float32 [64, 1024, 1024], P('fsdp', None, 'dp'), may hold values from -6 to 6
- right_statistic_matrix: float32 [64, 1024, 1024], P('fsdp', None, 'dp'), may hold values from -6 to 6
- first_adam_moment: float32 [64, 1024, 1024], P('fsdp', None, 'dp'), may hold values from -0.09 to 0.09
- second_adam_moment: float32 [64, 1024, 1024], P('fsdp', None, 'dp'), may hold values from 1e-05 to 0.001
Outputs:
- new_left_stat: float32 [64, 1024, 1024], P('fsdp', None, 'dp')
- new_right_stat: float32 [64, 1024, 1024], P('fsdp', None, 'dp')
- new_first: float32 [64, 1024, 1024], P('fsdp', None, 'dp')
- new_second: float32 [64, 1024, 1024], P('fsdp', None, 'dp')
- update: bfloat16 [4096, 8, 1024], P('fsdp', None, 'dp')
The draws below stay inside these ranges and needn't reach their ends.
Inputs may be any that keep to these rules, and one draw needn't show every extreme that they name: `block_owner_index`: no fsdp index owns more than 2 blocks; a quarter of the fsdp indices own 2 blocks and a quarter own none.
All inputs are finite; a program needn't handle non-finite values.
Results may differ from the reference program's by a relative error of at most 0.013.
Values may be sent and summed in bfloat16 or wider, within the bound.
No kernel may reach another device: no remote copies, remote signals or barrier semaphores. Data moves between devices by JAX's collectives and lax.ppermute only.
A program may use at most 128 MiB of HBM per device.

```python
import math
import jax
import jax.numpy as jnp
from jax import lax

BLOCK_ORDER = 1024
ROWS = 4096
SLOTS = 2
NBC = 8
NBLK = 32
SLOT_TOTAL = 64
N_DP = 4
N_FSDP = 32


def draw_block_owner_index(key, part):
    first_key, second_key = jax.random.split(jax.random.fold_in(key, 7))
    order = jax.random.permutation(first_key, N_FSDP)
    heavy = N_FSDP // 4
    places = jnp.arange(N_FSDP, dtype=jnp.int32)
    position = jnp.where(places < 2 * heavy, places // 2, places - heavy)
    listed = order[position]
    shuffle = jax.random.permutation(second_key, N_FSDP)
    return listed[shuffle].astype(jnp.int32)


def draw_gradient(key, part):
    keys = jax.random.split(jax.random.fold_in(key, 11), 4)
    sigma = 3.5 / math.sqrt(BLOCK_ORDER)
    factors = 4
    noise = jax.random.normal(keys[0], (N_DP, ROWS, NBC, BLOCK_ORDER), jnp.float32) * (sigma / math.sqrt(N_DP))
    picked = jax.random.permutation(keys[1], N_DP)
    quarter = jnp.arange(BLOCK_ORDER, dtype=jnp.int32) // (BLOCK_ORDER // N_DP)
    boost = jnp.where(quarter[None, :] == picked[:, None], 2.5, 1.0).astype(jnp.float32)
    noise = noise * boost[:, None, None, :]
    row_factor = jax.random.normal(keys[2], (ROWS, factors), jnp.float32)
    col_factor = jax.random.normal(keys[3], (factors, NBC, BLOCK_ORDER), jnp.float32)
    common = jnp.einsum('rk,knj->rnj', row_factor, col_factor) * (sigma / math.sqrt(factors))
    value = noise + common[None] / N_DP
    return jnp.clip(value, -3.0, 3.0).astype(jnp.bfloat16)


def steps_of(stream_key, dims, cuts, low, largest):
    factor_of = 1.0
    for dim, parts in cuts:
        heights = jax.random.uniform(jax.random.fold_in(jax.random.fold_in(stream_key, 6), dim), (parts,), jnp.float32, low / len(cuts), largest / len(cuts))
        factor_of = factor_of * jnp.repeat(jnp.exp(heights), dims[dim] // parts).reshape((-1,) + (1,) * (len(dims) - 1 - dim))
    return factor_of


def normal_values(rng, extent, scale, bound, shards=(), held_as=jnp.bfloat16):
    values = jax.random.normal(rng, extent, jnp.float32) * scale
    if len(shards) > 0:
        values = steps_of(rng, extent, shards, -0.22, 0.18) * values
    return jnp.clip(values, min=-bound, max=bound).astype(held_as)


def setup_inputs(seed: int = 0) -> dict:
    streams_of = jax.random.split(jax.random.key(seed), 10)
    return {
        "gradient": draw_gradient(jax.random.fold_in(streams_of[9], 71), 0),
        "block_owner_index": draw_block_owner_index(jax.random.fold_in(streams_of[9], 71), 0),
        "block_grid_cell": jax.random.permutation(streams_of[2], NBLK).astype(jnp.int32),
        "left_eigen_basis": normal_values(streams_of[3], (SLOT_TOTAL, BLOCK_ORDER, BLOCK_ORDER), BLOCK_ORDER ** -0.5, 0.1875, ((0, 32), (2, 4)), jnp.float32),
        "right_eigen_basis": normal_values(streams_of[4], (SLOT_TOTAL, BLOCK_ORDER, BLOCK_ORDER), BLOCK_ORDER ** -0.5, 0.1875, ((0, 32), (2, 4)), jnp.float32),
        "left_statistic_matrix": normal_values(streams_of[5], (SLOT_TOTAL, BLOCK_ORDER, BLOCK_ORDER), 1.0, 6.0, ((0, 32), (2, 4)), jnp.float32),
        "right_statistic_matrix": normal_values(streams_of[6], (SLOT_TOTAL, BLOCK_ORDER, BLOCK_ORDER), 1.0, 6.0, ((0, 32), (2, 4)), jnp.float32),
        "first_adam_moment": normal_values(streams_of[7], (SLOT_TOTAL, BLOCK_ORDER, BLOCK_ORDER), 0.015, 0.09, ((0, 32), (2, 4)), jnp.float32),
        "second_adam_moment": jnp.clip(jnp.exp(math.log(0.001) - 4.6051703 * jax.random.uniform(streams_of[8], (SLOT_TOTAL, BLOCK_ORDER, BLOCK_ORDER), jnp.float32) ** steps_of(streams_of[8], (SLOT_TOTAL, BLOCK_ORDER, BLOCK_ORDER), ((0, 32), (2, 4)), -0.2, 0.2)), 9.999999747378752e-06, 0.001),
    }


def slot_lookup_table(block_owner_index, block_grid_cell, slot_count):
    block_ids = jnp.arange(block_owner_index.shape[0], dtype=jnp.int32)
    shared = (block_owner_index[:, None] == block_owner_index[None, :]) & (block_ids[None, :] < block_ids[:, None])
    rank_in = lax.optimization_barrier(jnp.sum(shared.astype(jnp.int32), axis=1))
    block_slot_index = block_owner_index * SLOTS + rank_in
    slot_ids = jnp.arange(slot_count, dtype=jnp.int32)
    matches = (block_slot_index[None, :] == slot_ids[:, None]).astype(jnp.int32)
    filled_marker = lax.optimization_barrier(jnp.sum(matches, axis=1))
    slot_grid_cell = lax.optimization_barrier(jnp.sum(matches * block_grid_cell[None, :], axis=1))
    return (block_slot_index, filled_marker, slot_grid_cell)

def reference(gradient, block_owner_index, block_grid_cell, left_eigen_basis, right_eigen_basis, left_statistic_matrix, right_statistic_matrix, first_adam_moment, second_adam_moment):
    highest = lax.Precision.HIGHEST
    summed = lax.optimization_barrier(jnp.sum(gradient.astype(jnp.float32), axis=0)).astype(jnp.bfloat16)
    grid_rows = ROWS // BLOCK_ORDER
    blocks = summed.reshape(grid_rows, BLOCK_ORDER, NBC, BLOCK_ORDER)
    block_slot_index, filled_marker, slot_grid_cell = slot_lookup_table(block_owner_index, block_grid_cell, SLOT_TOTAL)
    anchor = jnp.zeros((), jnp.int32)

    def one_slot(items):
        filled_one, cell_one, left_one, right_one, lstat, rstat, first_one, second_one = items
        row_at = (cell_one // NBC).astype(jnp.int32)
        col_at = (cell_one % NBC).astype(jnp.int32)
        piece = lax.dynamic_slice(blocks, (row_at, anchor, col_at, anchor), (1, BLOCK_ORDER, 1, BLOCK_ORDER)).reshape(BLOCK_ORDER, BLOCK_ORDER)
        piece = jnp.where(filled_one > 0, piece, jnp.zeros_like(piece))
        new_left = 0.95 * lstat + 0.05 * jnp.dot(piece, piece.T, preferred_element_type=jnp.float32)
        new_right = 0.95 * rstat + 0.05 * jnp.dot(piece.T, piece, preferred_element_type=jnp.float32)
        half_turn = jnp.dot(left_one.T, piece.astype(jnp.float32), precision=highest).astype(jnp.bfloat16)
        turned = jnp.dot(half_turn.astype(jnp.float32), right_one, precision=highest)
        new_first = 0.9 * first_one + 0.1 * turned
        new_second = 0.999 * second_one + 0.001 * turned * turned
        direction = new_first / (jnp.sqrt(new_second) + 1e-08)
        mixed = jnp.dot(direction, right_one.T, precision=highest)
        back = jnp.dot(left_one, mixed, precision=highest).astype(jnp.bfloat16)
        return (new_left, new_right, new_first, new_second, back)
    new_left, new_right, new_first, new_second, backs = lax.map(one_slot, (filled_marker, slot_grid_cell, left_eigen_basis, right_eigen_basis, left_statistic_matrix, right_statistic_matrix, first_adam_moment, second_adam_moment))
    cells = jnp.arange(NBLK, dtype=jnp.int32)
    cell_hits = (block_grid_cell[None, :] == cells[:, None]).astype(jnp.int32)
    slot_for_cell = lax.optimization_barrier(jnp.sum(cell_hits * block_slot_index[None, :], axis=1))
    picked = jnp.take(backs, slot_for_cell, axis=0)
    update = picked.reshape(grid_rows, NBC, BLOCK_ORDER, BLOCK_ORDER).transpose(0, 2, 1, 3).reshape(ROWS, NBC, BLOCK_ORDER)
    return (new_left, new_right, new_first, new_second, update)
```

```python
import jax
import jax.numpy as jnp
from jax import lax
from jax.sharding import Mesh, PartitionSpec as P

BF = jnp.bfloat16
F32 = jnp.float32


def shift(x, by, n):
    return lax.ppermute(x, "dp", [(i, (i + by) % n) for i in range(n)])


def place(parts, me, n):
    width = parts[0].shape[-1]
    own, left, right, across = parts
    out = jnp.zeros(own.shape[:-1] + (n * width,), own.dtype)
    for piece, by in ((own, 0), (left, n - 1), (right, 1), (across, 2)):
        at = lax.rem(me + by, n) * width
        out = lax.dynamic_update_slice_in_dim(out, piece, at, out.ndim - 1)
    return out


def gather_columns(x, me, n):
    left = shift(x, 1, n)
    right = shift(x, n - 1, n)
    a = shift(left[0], 1, n)
    b = shift(right[1], n - 1, n)
    across = jnp.stack([a, b])
    return place((x, left, right, across), me, n)


def slot_tables(owner, cell, slot_count, per_owner):
    ids = jnp.arange(owner.shape[0], dtype=jnp.int32)
    shared = (owner[:, None] == owner[None, :]) & (ids[None, :] < ids[:, None])
    rank = jnp.sum(shared.astype(jnp.int32), axis=1)
    block_slot = owner * per_owner + rank
    slot_ids = jnp.arange(slot_count, dtype=jnp.int32)
    match = (block_slot[None, :] == slot_ids[:, None]).astype(jnp.int32)
    filled = jnp.sum(match, axis=1)
    slot_cell = jnp.sum(match * cell[None, :], axis=1)
    cells = jnp.arange(owner.shape[0], dtype=jnp.int32)
    hit = (cell[None, :] == cells[:, None]).astype(jnp.int32)
    cell_slot = jnp.sum(hit * block_slot[None, :], axis=1)
    return filled, slot_cell, cell_slot


def local(gradient, owner, cell, left_basis, right_basis, left_stat, right_stat, first, second):
    n = lax.axis_size("dp")
    me = lax.axis_index("dp")
    grid_rows = lax.axis_size("gr")
    bands = lax.axis_size("band")
    members = grid_rows * bands
    per_owner, block, width = left_basis.shape
    band_rows, grid_cols = gradient.shape[1], gradient.shape[2]
    piece = band_rows // grid_rows
    slot_count = per_owner * members
    half = band_rows // 2
    g = gradient[0]

    def chunk(by):
        return lax.dynamic_slice_in_dim(g, lax.rem(me + by, n) * width, width, 2)

    def added(x, y):
        return (x.astype(F32) + y.astype(F32)).astype(BF)

    filled, slot_cell, cell_slot = slot_tables(owner, cell, slot_count, per_owner)
    across = chunk(2)
    from_left = shift(across[:half], 1, n)
    from_right = shift(across[half:], n - 1, n)
    to_right, to_left = chunk(1), chunk(n - 1)
    to_right = jnp.concatenate([added(to_right[:half], from_left), to_right[half:]])
    to_left = jnp.concatenate([to_left[:half], added(to_left[half:], from_right)])
    in_left = shift(to_right, 1, n)
    in_right = shift(to_left, n - 1, n)
    summed = (chunk(0).astype(F32) + in_left.astype(F32) + in_right.astype(F32)).astype(BF)

    left_bf, summed = lax.optimization_barrier((left_basis.astype(BF), summed))
    right_bf = right_basis.astype(BF)
    full_left = gather_columns(left_bf, me, n)

    spread = lax.all_to_all(
        summed.reshape(grid_rows, piece, grid_cols, width), "gr", 0, 0, tiled=True
    )
    by_cell = jnp.transpose(spread, (0, 2, 1, 3)).reshape(grid_rows * grid_cols, piece, width)
    leaving = jnp.take(by_cell, slot_cell, axis=0)
    leaving = jnp.where((filled > 0)[:, None, None], leaving, jnp.zeros_like(leaving))
    landed = lax.all_to_all(
        leaving.reshape(members, per_owner, piece, width), ("gr", "band"), 0, 0, tiled=True
    )
    landed = landed.reshape(grid_rows, bands, per_owner, piece, width)
    mine = jnp.transpose(landed, (2, 1, 0, 3, 4)).reshape(per_owner, block, width)
    grad = gather_columns(mine, me, n)

    z = jnp.einsum("sij,sjc->sic", grad, right_bf, preferred_element_type=F32).astype(BF)
    turned = jnp.einsum("sik,sic->skc", full_left, z, preferred_element_type=F32)
    new_first = 0.9 * first + 0.1 * turned
    new_second = 0.999 * second + 0.001 * turned * turned
    direction = (new_first / (jnp.sqrt(new_second) + 1e-8)).astype(BF)
    applied = jnp.einsum("sik,skc->sic", full_left, direction, preferred_element_type=F32).astype(BF)

    def partial(by):
        rows = lax.dynamic_slice_in_dim(right_bf, lax.rem(me + by, n) * width, width, 1)
        return jnp.einsum("sic,sjc->sij", applied, rows, preferred_element_type=F32)

    across = partial(2).astype(BF)
    from_left = shift(across[0], 1, n)
    from_right = shift(across[1], n - 1, n)
    to_right, to_left = partial(1), partial(n - 1)
    to_right = jnp.stack([(to_right[0] + from_left.astype(F32)).astype(BF), to_right[1].astype(BF)])
    to_left = jnp.stack([to_left[0].astype(BF), (to_left[1] + from_right.astype(F32)).astype(BF)])
    in_left = shift(to_right, 1, n)
    in_right = shift(to_left, n - 1, n)
    back = (partial(0) + in_left.astype(F32) + in_right.astype(F32)).astype(BF)

    parted = back.reshape(per_owner, bands, grid_rows, piece, width)
    parted = jnp.transpose(parted, (2, 1, 0, 3, 4)).reshape(members, per_owner, piece, width)
    homed = lax.all_to_all(parted, ("gr", "band"), 0, 0, tiled=True)
    homed = homed.reshape(slot_count, piece, width)
    per_cell = jnp.take(homed, cell_slot, axis=0).reshape(grid_rows, grid_cols, piece, width)
    final = lax.all_to_all(per_cell, "gr", 0, 0, tiled=True)
    update = jnp.transpose(final, (0, 2, 1, 3)).reshape(band_rows, grid_cols, width)

    rows = lax.dynamic_slice_in_dim(grad, me * width, width, 1)
    new_left = 0.95 * left_stat + 0.05 * jnp.einsum(
        "sik,sjk->sij", grad, rows, preferred_element_type=F32
    )
    new_right = 0.95 * right_stat + 0.05 * jnp.einsum(
        "ski,skj->sij", grad, mine, preferred_element_type=F32
    )
    return new_left, new_right, new_first, new_second, update


def solution(mesh):
    n, members = mesh.shape["dp"], mesh.shape["fsdp"]

    def run(gradient, owner, cell, *state):
        bands = state[0].shape[1] // (gradient.shape[1] // members)
        inner = Mesh(mesh.devices.reshape(n, members // bands, bands), ("dp", "gr", "band"))
        fsdp = ("gr", "band")
        part = P(fsdp, None, "dp")
        f = jax.shard_map(
            local,
            mesh=inner,
            in_specs=(P("dp", fsdp, None, None), P(), P()) + (part,) * 6,
            out_specs=(part,) * 5,
            check_vma=False,
        )
        return f(gradient, owner, cell, *state)

    return run
```

```python
import functools

import jax
import jax.numpy as jnp
from jax import lax
from jax.experimental import pallas as pl
from jax.experimental.pallas import tpu as pltpu
from jax.sharding import Mesh, PartitionSpec as P


BF = jnp.bfloat16
F32 = jnp.float32
TILE = 512
VMEM_TURN = 60 * 2**20


def shift(x, by, n):
    return lax.ppermute(x, "dp", [(i, (i + by) % n) for i in range(n)])


def dot(x, y, dims):
    return lax.dot_general(x, y, (dims, ((), ())), preferred_element_type=F32)


NN = ((1,), (0,))
NT = ((1,), (1,))
TN = ((0,), (0,))


def rows_at(me, by, n, size):
    return pl.ds(pl.multiple_of(lax.rem(me + by, n) * size, size), size)


def flip_kernel(*refs):
    ins, out, buf, res, sems, out_sems = refs[:4], *refs[4:]
    width = buf.shape[2]
    copies = []
    for k, ref in enumerate(ins):
        c = pltpu.make_async_copy(ref, buf.at[k], sems.at[k])
        c.start()
        copies.append(c)
    stores = []
    for k in range(4):
        copies[k].wait()
        res[k] = buf[k].T
        c = pltpu.make_async_copy(res.at[k], out.at[pl.ds(k * width, width)], out_sems.at[k])
        c.start()
        stores.append(c)
    for c in stores:
        c.wait()


def flip(lb):
    block, width = lb[0].shape
    anyspec = pl.BlockSpec(memory_space=pltpu.HBM)
    return pl.pallas_call(
        flip_kernel,
        out_shape=jax.ShapeDtypeStruct((block, block), BF),
        in_specs=[anyspec] * 4,
        out_specs=anyspec,
        scratch_shapes=[
            pltpu.VMEM((4, block, width), BF),
            pltpu.VMEM((4, width, block), BF),
            pltpu.SemaphoreType.DMA((4,)),
            pltpu.SemaphoreType.DMA((4,)),
        ],
        compiler_params=pltpu.CompilerParams(vmem_limit_bytes=VMEM_TURN),
        cost_estimate=pl.CostEstimate(flops=2**22, bytes_accessed=4 * 2**20, transcendentals=0),
        name="flip",
    )(*lb)


def turn_kernel(n, s, *refs):
    me_ref = refs[0]
    g_own, g_left, g_right, g_top, g_bottom = refs[1:6]
    l_parts, lt_hbm = refs[6:10], refs[10]
    r_hbm, first_hbm, second_hbm = refs[11:14]
    (nf_hbm, ns_hbm, g_out, own_out, far_t, far_b, right_t, right_b, left_t, left_b) = refs[-23:-13]
    g, lb, lt, r, first, second, z, d, t, p, sems, out_sems, _ = refs[-13:]
    me = me_ref[0]
    _, pieces, piece, block = g.shape
    width = z.shape[1]
    half = pieces // 2
    loads, stores = [], []

    def load(src, dst):
        c = pltpu.make_async_copy(src, dst, sems.at[len(loads)])
        c.start()
        loads.append(c)
        return c

    def store(src, dst):
        c = pltpu.make_async_copy(src, dst, out_sems.at[len(stores)])
        c.start()
        stores.append(c)

    def cols(k):
        return pl.ds(k * width, width)

    offsets = (0, n - 1, 1, 2)
    w_g = [
        load(r_hbm.at[s, rows_at(me, offsets[k], n, width), :], r.at[cols(k), :]) for k in range(4)
    ]
    for k, ref in enumerate((g_own, g_left, g_right)):
        w_g += [load(ref.at[q], g.at[:, q, :, cols(k)]) for q in range(pieces)]
    for q in range(half):
        w_g.append(load(g_top.at[q], g.at[:, q, :, cols(3)]))
        w_g.append(load(g_bottom.at[q], g.at[:, q + half, :, cols(3)]))
    w_lt = load(lt_hbm, lt)
    w_m = [load(first_hbm.at[s], first), load(second_hbm.at[s], second)]
    w_l = [load(ref, lb.at[:, cols(k)]) for k, ref in enumerate(l_parts)]

    per = TILE // (pieces * piece)
    tiles = block // TILE
    for c in w_g:
        c.wait()
    store(g, g_out)

    @pl.loop(0, tiles)
    def _(i):
        rows = g[pl.ds(i * per, per)].reshape(TILE, block)
        at = pl.ds(pl.multiple_of(i * TILE, TILE), TILE)
        z[at, :] = dot(rows, r[...], NN).astype(BF)

    w_lt.wait()
    for c in w_m:
        c.wait()
    for k in range(4):
        at = rows_at(me, offsets[k], n, width)
        turned = dot(lt[cols(k), :], z[...], NN)
        nf = 0.9 * first[at, :] + 0.1 * turned
        ns = 0.999 * second[at, :] + 0.001 * turned * turned
        first[at, :] = nf
        second[at, :] = ns
        d[cols(k), :] = (nf / (jnp.sqrt(ns) + 1e-8)).astype(BF)
    store(first, nf_hbm.at[s])
    store(second, ns_hbm.at[s])
    for c in w_l:
        c.wait()

    @pl.loop(0, tiles)
    def _(i):
        at = pl.ds(pl.multiple_of(i * TILE, TILE), TILE)
        t[at, :] = dot(lb[at, :], d[...], NN).astype(BF)

    for k in (3, 2, 1, 0):

        @pl.loop(0, tiles)
        def _(i):
            at = pl.ds(pl.multiple_of(i * TILE, TILE), TILE)
            v = dot(t[at, :], r[cols(k), :], NT).astype(BF)
            p[pl.ds(i * per, per), :, :, cols(k)] = v.reshape(per, pieces, piece, width)

        for q in range(pieces):
            src = p.at[:, q, :, cols(k)]
            if k == 0:
                store(src, own_out.at[q])
            else:
                top, bottom = {3: (far_t, far_b), 2: (right_t, right_b), 1: (left_t, left_b)}[k]
                store(src, top.at[q] if q < half else bottom.at[q - half])
    for c in stores:
        c.wait()


def turn(me, s, g, lb, lt, r, first, second, before, n):
    _, block, width = r.shape
    pieces, bands, piece, _ = g[0].shape
    anyspec = pl.BlockSpec(memory_space=pltpu.HBM)
    state = jax.ShapeDtypeStruct(first.shape, F32)
    whole = jax.ShapeDtypeStruct(g[0].shape, BF)
    part = jax.ShapeDtypeStruct(g[3].shape, BF)
    full = jax.ShapeDtypeStruct((bands, pieces, piece, block), BF)
    return pl.pallas_call(
        functools.partial(turn_kernel, n, s),
        out_shape=[state, state, full, whole] + [part] * 6,
        in_specs=[pl.BlockSpec(memory_space=pltpu.SMEM)] + [anyspec] * (13 + len(before)),
        out_specs=[anyspec] * 10,
        scratch_shapes=[
            pltpu.VMEM((bands, pieces, piece, block), BF),
            pltpu.VMEM((block, block), BF),
            pltpu.VMEM((block, block), BF),
            pltpu.VMEM((block, width), BF),
            pltpu.VMEM((block, width), F32),
            pltpu.VMEM((block, width), F32),
            pltpu.VMEM((block, width), BF),
            pltpu.VMEM((block, width), BF),
            pltpu.VMEM((block, width), BF),
            pltpu.VMEM((bands, pieces, piece, block), BF),
            pltpu.SemaphoreType.DMA((27,)),
            pltpu.SemaphoreType.DMA((19,)),
            pltpu.SMEM((1,), jnp.int32),
        ],
        input_output_aliases={14 + i: i for i in range(len(before))},
        compiler_params=pltpu.CompilerParams(vmem_limit_bytes=VMEM_TURN),
        cost_estimate=pl.CostEstimate(
            flops=8 * block * block * width, bytes_accessed=14 * 2**20, transcendentals=0
        ),
        name="turn",
    )(me, *g, *lb, lt, r, first, second, *before)


def stats_kernel(n, me_ref, g, lstat, rstat, *rest):
    new_l, new_r = rest[-2:]
    me = me_ref[0]
    block = g.shape[0]
    width = lstat.shape[2]

    @pl.loop(0, block // TILE)
    def _(i):
        at = pl.ds(pl.multiple_of(i * TILE, TILE), TILE)
        acc = dot(g[at, :], g[rows_at(me, 0, n, width), :], NT)
        new_l[0, at, :] = 0.95 * lstat[0, at, :] + 0.05 * acc

    for k, by in enumerate((0, n - 1, 1, 2)):
        at = rows_at(me, by, n, width)
        acc = dot(g[:, k * width : (k + 1) * width], g[:, :width], TN)
        new_r[0, at, :] = 0.95 * rstat[0, at, :] + 0.05 * acc


def stats(me, s, g, lstat, rstat, before, n):
    _, block, width = lstat.shape
    slot = pl.BlockSpec((1, block, width), lambda i: (s, 0, 0))
    anyspec = pl.BlockSpec(memory_space=pltpu.HBM)
    out = jax.ShapeDtypeStruct(lstat.shape, F32)
    return pl.pallas_call(
        functools.partial(stats_kernel, n),
        grid=(1,),
        out_shape=[out, out],
        in_specs=[
            pl.BlockSpec(memory_space=pltpu.SMEM),
            pl.BlockSpec((block, block), lambda i: (0, 0)),
            slot,
            slot,
        ]
        + [anyspec] * len(before),
        out_specs=[slot, slot],
        input_output_aliases={4 + i: i for i in range(len(before))},
        compiler_params=pltpu.CompilerParams(vmem_limit_bytes=24 * 2**20),
        cost_estimate=pl.CostEstimate(
            flops=4 * block * block * width, bytes_accessed=6 * 2**20, transcendentals=0
        ),
        name="stats",
    )(me, g.reshape(block, block), lstat, rstat, *before)


def finish_kernel(*refs):
    out = refs[-1]

    def total(x, y, z):
        return (x.astype(F32) + y.astype(F32) + z.astype(F32)).astype(BF)

    for s in range(2):
        own, left_t, left_b, right_t, right_b = refs[5 * s : 5 * s + 5]
        half = left_t.shape[0]
        for q in range(half):
            out[q, :, s] = total(own[q], left_t[q], right_t[q])
            out[q + half, :, s] = total(own[q + half], left_b[q], right_b[q])


def finish(parts):
    pieces, bands, piece, width = parts[0].shape
    return pl.pallas_call(
        finish_kernel,
        out_shape=jax.ShapeDtypeStruct((pieces, bands, 2, piece, width), BF),
        in_specs=[pl.BlockSpec(memory_space=pltpu.VMEM)] * 10,
        out_specs=pl.BlockSpec(memory_space=pltpu.VMEM),
        compiler_params=pltpu.CompilerParams(vmem_limit_bytes=VMEM_TURN),
        cost_estimate=pl.CostEstimate(flops=2**20, bytes_accessed=4 * 2**20, transcendentals=0),
        name="finish",
    )(*parts)


def gather_pair(x, n):
    left0 = shift(x[0], 1, n)
    right1 = shift(x[1], n - 1, n)
    left1 = shift(x[1], 1, n)
    right0 = shift(x[0], n - 1, n)
    across0 = shift(left0, 1, n)
    across1 = shift(right1, n - 1, n)
    return (x[0], left0, right0, across0), (x[1], left1, right1, across1)


def gather_columns(x, n):
    half = x.shape[0] // 2
    left = shift(x, 1, n)
    right = shift(x, n - 1, n)
    top = shift(left[:half], 1, n)
    bottom = shift(right[half:], n - 1, n)
    return x, left, right, top, bottom


def slot_tables(owner, cell, members, per_owner):
    ids = jnp.arange(owner.shape[0], dtype=jnp.int32)
    shared = (owner[:, None] == owner[None, :]) & (ids[None, :] < ids[:, None])
    rank = jnp.sum(shared.astype(jnp.int32), axis=1)
    block_slot = owner * per_owner + rank
    slot_ids = jnp.arange(per_owner * members, dtype=jnp.int32)
    match = (block_slot[None, :] == slot_ids[:, None]).astype(jnp.int32)
    filled = jnp.sum(match, axis=1)
    slot_cell = jnp.sum(match * cell[None, :], axis=1)
    cells = jnp.arange(owner.shape[0], dtype=jnp.int32)
    hit = (cell[None, :] == cells[:, None]).astype(jnp.int32)
    cell_slot = jnp.sum(hit * block_slot[None, :], axis=1)
    return filled, slot_cell, cell_slot


def added(*xs):
    return sum(x.astype(F32) for x in xs).astype(BF)


def local(gradient, owner, cell, left_basis, right_basis, left_stat, right_stat, first, second):
    n = lax.axis_size("dp")
    me = lax.axis_index("dp")
    grid_rows = lax.axis_size("gr")
    bands = lax.axis_size("band")
    members = grid_rows * bands
    per_owner, _, width = left_basis.shape
    band_rows, grid_cols = gradient.shape[1], gradient.shape[2]
    piece = band_rows // grid_rows
    half = band_rows // 2
    g = gradient[0]

    def chunk(by, lo, hi):
        return lax.dynamic_slice(
            g, (lo, 0, lax.rem(me + by, n) * width), (hi - lo, grid_cols, width)
        )

    filled, slot_cell, cell_slot = slot_tables(owner, cell, members, per_owner)
    from_left = shift(chunk(2, 0, half), 1, n)
    from_right = shift(chunk(2, half, band_rows), n - 1, n)
    in_left_b = shift(chunk(1, half, band_rows), 1, n)
    in_right_a = shift(chunk(n - 1, 0, half), n - 1, n)
    right_sum = added(chunk(1, 0, half), from_left)
    left_sum = added(chunk(n - 1, half, band_rows), from_right)
    in_left_a = shift(right_sum, 1, n)
    in_right_b = shift(left_sum, n - 1, n)
    summed = jnp.concatenate(
        [
            added(chunk(0, 0, half), in_left_a, in_right_a),
            added(chunk(0, half, band_rows), in_left_b, in_right_b),
        ]
    )

    right_bf = right_basis.astype(BF)
    pieces_l = gather_pair([left_basis[s].astype(BF) for s in range(2)], n)

    spread = lax.all_to_all(
        summed.reshape(grid_rows, piece, grid_cols, width), "gr", 0, 0, tiled=True
    )
    by_cell = jnp.transpose(spread, (0, 2, 1, 3)).reshape(grid_rows * grid_cols, piece, width)
    leaving = jnp.take(by_cell, slot_cell, axis=0, mode="clip")
    leaving = jnp.where((filled > 0)[:, None, None], leaving, jnp.zeros_like(leaving))
    landed = lax.all_to_all(
        leaving.reshape(members, per_owner, piece, width), ("gr", "band"), 0, 0, tiled=True
    )
    landed = landed.reshape(grid_rows, bands, per_owner, piece, width)
    pieces_g = [gather_columns(landed[:, :, s], n) for s in range(per_owner)]

    me_s = me.reshape(1).astype(jnp.int32)
    state, fulls, terms = (), [], []
    flipped = []
    for s in range(per_owner):
        flipped.append(flip(pieces_l[s]))
    for s in range(per_owner):
        nf, ns, full, own, *parts = turn(
            me_s, s, pieces_g[s], pieces_l[s], flipped[s], right_bf, first, second, state, n
        )
        state = (nf, ns)
        fulls.append(full)
        far_t, far_b, right_t, right_b, left_t, left_b = parts
        from_left = shift(far_t, 1, n)
        from_right = shift(far_b, n - 1, n)
        in_left_b = shift(right_b, 1, n)
        in_right_t = shift(left_t, n - 1, n)
        right_sum, left_sum = added(right_t, from_left), added(left_b, from_right)
        in_left_t = shift(right_sum, 1, n)
        in_right_b = shift(left_sum, n - 1, n)
        terms += [own, in_left_t, in_left_b, in_right_t, in_right_b]
    homed = lax.all_to_all(
        finish(terms).reshape(members, per_owner, piece, width),
        ("gr", "band"), 0, 0, tiled=True,
    )
    per_cell = jnp.take(
        homed.reshape(members * per_owner, piece, width), cell_slot, axis=0, mode="clip"
    )
    final = lax.all_to_all(
        per_cell.reshape(grid_rows, grid_cols, piece, width), "gr", 0, 0, tiled=True
    )
    update = jnp.transpose(final, (0, 2, 1, 3)).reshape(band_rows, grid_cols, width)

    done = ()
    for s in range(per_owner):
        done = stats(me_s, s, fulls[s], left_stat, right_stat, done, n)
    return tuple(done) + state + (update,)


def solution(mesh):
    n, members = mesh.shape["dp"], mesh.shape["fsdp"]

    def run(gradient, owner, cell, *state):
        bands = state[0].shape[1] // (gradient.shape[1] // members)
        inner = Mesh(mesh.devices.reshape(n, members // bands, bands), ("dp", "gr", "band"))
        fsdp = ("gr", "band")
        part = P(fsdp, None, "dp")

        f = jax.shard_map(
            local,
            mesh=inner,
            in_specs=(P("dp", fsdp, None, None), P(), P()) + (part,) * 6,
            out_specs=(part,) * 5,
            check_vma=False,
        )
        return f(gradient, owner, cell, *state)

    return run
```

```python
import functools

import jax
import jax.numpy as jnp
from jax import lax
from jax.experimental import pallas as pl
from jax.experimental.pallas import tpu as pltpu
from jax.sharding import Mesh, PartitionSpec as P


BF = jnp.bfloat16
F32 = jnp.float32
TILE = 1024
VMEM_TURN = 20 * 2**20


def shift(x, by, n):
    return lax.ppermute(x, "dp", [(i, (i + by) % n) for i in range(n)])


def dot(x, y, dims):
    return lax.dot_general(x, y, (dims, ((), ())), preferred_element_type=F32)


NN = ((1,), (0,))
NT = ((1,), (1,))
TN = ((0,), (0,))


def rows_at(me, by, n, size):
    return pl.ds(pl.multiple_of(lax.rem(me + by, n) * size, size), size)


OFFSETS = (0, 3, 1, 2)


def in_vmem(x):
    return pltpu.with_memory_space_constraint(x, pltpu.MemorySpace.VMEM)


def in_hbm(x):
    return pltpu.with_memory_space_constraint(x, pltpu.MemorySpace.HBM)


def starter(sems):
    started = []

    def start(src, dst):
        c = pltpu.make_async_copy(src, dst, sems.at[len(started)])
        c.start()
        started.append(c)
        return c

    return start, started


def cols(k, width):
    return pl.ds(k * width, width)


def prep_kernel(n, s, count, *refs):
    me_ref = refs[0]
    l_parts = refs[1 : 1 + count]
    r_hbm, first_hbm, second_hbm = refs[1 + count : 4 + count]
    lb, lt, r, first, second, sems = refs[-6:]
    me = me_ref[0]
    width = r.shape[1]
    tall = lb.shape[0] // 2
    load, loads = starter(sems)
    for k in range(3):
        load(l_parts[k], lb.at[:, cols(k, width)])
    if count == 4:
        load(l_parts[3], lb.at[:, cols(3, width)])
    else:
        load(l_parts[3], lb.at[pl.ds(0, tall), cols(3, width)])
        load(l_parts[4], lb.at[pl.ds(tall, tall), cols(3, width)])
    for k in range(4):
        load(r_hbm.at[s, rows_at(me, OFFSETS[k], n, width), :], r.at[cols(k, width), :])
    load(first_hbm.at[s], first)
    load(second_hbm.at[s], second)
    for k in range(4):
        loads[k].wait()
        if k == 3 and count == 5:
            loads[4].wait()
        lt[cols(k, width), :] = lb[:, cols(k, width)].T
    for c in loads[count:]:
        c.wait()


def prep(me, s, lb, r, first, second, after, n):
    _, block, width = r.shape
    hbm = pl.BlockSpec(memory_space=pltpu.HBM)
    vmem = pl.BlockSpec(memory_space=pltpu.VMEM)
    return pl.pallas_call(
        functools.partial(prep_kernel, n, s, len(lb)),
        out_shape=[
            pltpu.VMEM((block, block), BF),
            pltpu.VMEM((block, block), BF),
            pltpu.VMEM((block, width), BF),
            pltpu.VMEM((block, width), F32),
            pltpu.VMEM((block, width), F32),
        ],
        in_specs=[pl.BlockSpec(memory_space=pltpu.SMEM)] + [hbm] * (3 + len(lb)) + [vmem] * len(after),
        out_specs=[vmem] * 5,
        scratch_shapes=[pltpu.SemaphoreType.DMA((11,))],
        compiler_params=pltpu.CompilerParams(vmem_limit_bytes=20 * 2**20),
        cost_estimate=pl.CostEstimate(flops=2**22, bytes_accessed=6 * 2**20, transcendentals=0),
        name="prep",
    )(me, *[in_hbm(x) for x in lb], in_hbm(r), in_hbm(first), in_hbm(second), *[in_vmem(x) for x in after])


def load_grad(load, s, parts, g, width, near=False):
    pieces = g.shape[1]
    half = pieces // 2
    waits = []
    if s == 0:
        for k, ref in enumerate(parts[:3]):
            waits += [load(ref.at[q], g.at[:, q, :, cols(k, width)]) for q in range(pieces)]
        for q in range(half):
            if near:
                g[:, q, :, 3 * width :] = parts[3][q]
                g[:, q + half, :, 3 * width :] = parts[4][q]
            else:
                waits.append(load(parts[3].at[q], g.at[:, q, :, cols(3, width)]))
                waits.append(load(parts[4].at[q], g.at[:, q + half, :, cols(3, width)]))
    elif near:
        for k in range(4):
            for q in range(pieces):
                g[:, q, :, k * width : (k + 1) * width] = parts[0][q, :, k]
    else:
        for k in range(4):
            waits += [
                load(parts[0].at[q, :, k], g.at[:, q, :, cols(k, width)]) for q in range(pieces)
            ]
    return waits


def turn_kernel(n, s, count, *refs):
    me_ref = refs[0]
    g_parts = refs[1 : 1 + count]
    lb, lt, r, first, second = refs[1 + count : 6 + count]
    nf_hbm, ns_hbm, own_out, to_right, to_left, right_t, left_b = refs[-16:-9]
    g, z, d, t, p, nf, ns, sems, out_sems = refs[-9:]
    me = me_ref[0]
    _, pieces, piece, block = g.shape
    width = z.shape[1]
    half = pieces // 2
    load, _ = starter(sems)
    store, stores = starter(out_sems)
    for c in load_grad(load, s, g_parts, g, width, near=True):
        c.wait()
    per = TILE // (pieces * piece)
    tiles = block // TILE

    @pl.loop(0, tiles)
    def _(i):
        rows = g[pl.ds(i * per, per)].reshape(TILE, block)
        at = pl.ds(pl.multiple_of(i * TILE, TILE), TILE)
        z[at, :] = dot(rows, r[...], NN).astype(BF)

    for k in range(4):
        at = rows_at(me, OFFSETS[k], n, width)
        turned = dot(lt[cols(k, width), :], z[...], NN)
        a = 0.9 * first[at, :] + 0.1 * turned
        b = 0.999 * second[at, :] + 0.001 * turned * turned
        nf[at, :] = a
        ns[at, :] = b
        d[cols(k, width), :] = (a / (jnp.sqrt(b) + 1e-8)).astype(BF)
    store(nf, nf_hbm.at[s])
    store(ns, ns_hbm.at[s])

    @pl.loop(0, tiles)
    def _(i):
        at = pl.ds(pl.multiple_of(i * TILE, TILE), TILE)
        t[at, :] = dot(lb[at, :], d[...], NN).astype(BF)

    for k in (3, 2, 1, 0):

        @pl.loop(0, tiles)
        def _(i):
            at = pl.ds(pl.multiple_of(i * TILE, TILE), TILE)
            v = dot(t[at, :], r[cols(k, width), :], NT).astype(BF)
            p[pl.ds(i * per, per), :, :, cols(k, width)] = v.reshape(per, pieces, piece, width)

        for q in range(pieces):
            src = p.at[:, q, :, cols(k, width)]
            low = q < half
            if k == 0:
                store(src, own_out.at[q])
            elif k == 3:
                store(src, to_right.at[q] if low else to_left.at[q - half])
            elif k == 2:
                store(src, right_t.at[q] if low else to_right.at[q])
            else:
                store(src, to_left.at[q + half] if low else left_b.at[q - half])
    for c in stores:
        c.wait()


def turn(me, s, g, ready, before, n, per_owner):
    block, width = ready[2].shape
    pieces, bands, piece = g[0].shape[0], g[0].shape[1], g[0].shape[-2]
    hbm = pl.BlockSpec(memory_space=pltpu.HBM)
    vmem = pl.BlockSpec(memory_space=pltpu.VMEM)
    far = 3 if s == 0 else 0
    state = pltpu.HBM((per_owner, block, width), F32)
    whole = pltpu.HBM((pieces, bands, piece, width), BF)
    part = pltpu.HBM((pieces // 2, bands, piece, width), BF)
    return pl.pallas_call(
        functools.partial(turn_kernel, n, s, len(g)),
        out_shape=[state, state, whole, whole, whole, part, part],
        in_specs=[pl.BlockSpec(memory_space=pltpu.SMEM)]
        + [hbm] * far
        + [vmem] * (len(g) - far)
        + [vmem] * 5
        + [hbm] * len(before),
        out_specs=[hbm] * 7,
        scratch_shapes=[
            pltpu.VMEM((bands, pieces, piece, block), BF),
            pltpu.VMEM((block, width), BF),
            pltpu.VMEM((block, width), BF),
            pltpu.VMEM((block, width), BF),
            pltpu.VMEM((bands, pieces, piece, block), BF),
            pltpu.VMEM((block, width), F32),
            pltpu.VMEM((block, width), F32),
            pltpu.SemaphoreType.DMA((16,)),
            pltpu.SemaphoreType.DMA((18,)),
        ],
        input_output_aliases={6 + len(g) + i: i for i in range(len(before))},
        compiler_params=pltpu.CompilerParams(vmem_limit_bytes=VMEM_TURN),
        cost_estimate=pl.CostEstimate(
            flops=8 * block * block * width, bytes_accessed=6 * 2**20, transcendentals=0
        ),
        name="turn",
    )(
        me,
        *[in_hbm(x) for x in g[:far]],
        *[in_vmem(x) for x in (*g[far:], *ready)],
        *[in_hbm(x) for x in before],
    )


def stats_kernel(n, s, count, *refs):
    me_ref = refs[0]
    g_parts = refs[1 : 1 + count]
    lstat, rstat = refs[1 + count : 3 + count]
    new_l, new_r, g, sems = refs[-4:]
    me = me_ref[0]
    _, _, _, block = g.shape
    width = lstat.shape[2]
    load, _ = starter(sems)
    for c in load_grad(load, s, g_parts, g, width):
        c.wait()
    flat = g.reshape(block, block)

    @pl.loop(0, block // TILE)
    def _(i):
        at = pl.ds(pl.multiple_of(i * TILE, TILE), TILE)
        acc = dot(flat[at, :], flat[rows_at(me, 0, n, width), :], NT)
        new_l[0, at, :] = 0.95 * lstat[0, at, :] + 0.05 * acc

    for k in range(4):
        at = rows_at(me, OFFSETS[k], n, width)
        acc = dot(flat[:, cols(k, width)], flat[:, cols(0, width)], TN)
        new_r[0, at, :] = 0.95 * rstat[0, at, :] + 0.05 * acc


def stats(me, s, g, lstat, rstat, before, n):
    _, block, width = lstat.shape
    pieces, bands, piece = g[0].shape[0], g[0].shape[1], g[0].shape[-2]
    slot = pl.BlockSpec((1, block, width), lambda i: (s, 0, 0))
    hbm = pl.BlockSpec(memory_space=pltpu.HBM)
    out = jax.ShapeDtypeStruct(lstat.shape, F32)
    return pl.pallas_call(
        functools.partial(stats_kernel, n, s, len(g)),
        grid=(1,),
        out_shape=[out, out],
        in_specs=[pl.BlockSpec(memory_space=pltpu.SMEM)]
        + [hbm] * len(g)
        + [slot, slot]
        + [hbm] * len(before),
        out_specs=[slot, slot],
        scratch_shapes=[
            pltpu.VMEM((bands, pieces, piece, block), BF),
            pltpu.SemaphoreType.DMA((16,)),
        ],
        input_output_aliases={3 + len(g) + i: i for i in range(len(before))},
        compiler_params=pltpu.CompilerParams(vmem_limit_bytes=24 * 2**20),
        cost_estimate=pl.CostEstimate(
            flops=4 * block * block * width, bytes_accessed=6 * 2**20, transcendentals=0
        ),
        name="stats",
    )(me, *[in_hbm(x) for x in g], lstat, rstat, *before)


def finish_kernel(s, *refs):
    own, from_left, from_right, in_left, in_right = refs[:5]
    out, a, b, sems, out_sems = refs[-5:]
    pieces = own.shape[0]
    half = pieces // 2
    load, loads = starter(sems)
    load(own, a)
    load(from_right.at[pl.ds(half, half)], b.at[pl.ds(0, half)])
    load(from_left.at[pl.ds(half, half)], b.at[pl.ds(half, half)])
    for x in loads:
        x.wait()
    store, stores = starter(out_sems)
    for q in range(pieces):
        c = in_left[q] if q < half else in_right[q - half]
        a[q] = (a[q].astype(F32) + b[q].astype(F32) + c.astype(F32)).astype(BF)
        store(a.at[q], out.at[q, :, s])
    for x in stores:
        x.wait()


def finish(s, own, from_left, from_right, in_left, in_right, before):
    pieces, bands, piece, width = own.shape
    hbm = pl.BlockSpec(memory_space=pltpu.HBM)
    vmem = pl.BlockSpec(memory_space=pltpu.VMEM)
    return pl.pallas_call(
        functools.partial(finish_kernel, s),
        out_shape=pltpu.HBM((pieces, bands, 2, piece, width), BF),
        in_specs=[hbm] * 3 + [vmem] * 2 + [hbm] * len(before),
        out_specs=hbm,
        scratch_shapes=[pltpu.VMEM(own.shape, BF)] * 2
        + [pltpu.SemaphoreType.DMA((3,)), pltpu.SemaphoreType.DMA((pieces,))],
        input_output_aliases={5 + i: i for i in range(len(before))},
        compiler_params=pltpu.CompilerParams(vmem_limit_bytes=16 * 2**20),
        cost_estimate=pl.CostEstimate(flops=2**20, bytes_accessed=2 * 2**20, transcendentals=0),
        name="finish",
    )(
        *[in_hbm(x) for x in (own, from_left, from_right)],
        in_vmem(in_left),
        in_vmem(in_right),
        *[in_hbm(x) for x in before],
    )


def gather_columns(x, n):
    half = x.shape[0] // 2
    left = shift(x, 1, n)
    right = shift(x, n - 1, n)
    top = shift(left[:half], 1, n)
    bottom = shift(right[half:], n - 1, n)
    return x, left, right, top, bottom


def slot_tables(owner, cell, members, per_owner, doubles):
    ids = jnp.arange(owner.shape[0], dtype=jnp.int32)
    shared = (owner[:, None] == owner[None, :]) & (ids[None, :] < ids[:, None])
    rank = jnp.sum(shared.astype(jnp.int32), axis=1)
    cells = jnp.arange(owner.shape[0], dtype=jnp.int32)
    hit = (cell[None, :] == cells[:, None]).astype(jnp.int32)
    cell_slot = jnp.sum(hit * (owner * per_owner + rank)[None, :], axis=1)
    who = jnp.arange(members, dtype=jnp.int32)
    mine = owner[None, :] == who[:, None]
    first = (mine & (rank == 0)[None, :]).astype(jnp.int32)
    second = (mine & (rank == 1)[None, :]).astype(jnp.int32)
    has_first = jnp.sum(first, axis=1)
    first_cell = jnp.sum(first * cell[None, :], axis=1)
    is_second = rank == 1
    before = jnp.sum((is_second[None, :] & (ids[None, :] < ids[:, None])).astype(jnp.int32), axis=1)
    place = jnp.where(is_second, before, doubles)
    second_place = jnp.sum(second * (place - doubles)[None, :], axis=1) + doubles
    spots = jnp.arange(doubles, dtype=jnp.int32)
    second_cell = jnp.sum((place[None, :] == spots[:, None]).astype(jnp.int32) * cell[None, :], axis=1)
    return has_first, first_cell, second_cell, second_place, cell_slot


def added(*xs):
    return sum(x.astype(F32) for x in xs).astype(BF)


def local(gradient, owner, cell, left_basis, right_basis, left_stat, right_stat, first, second):
    n = lax.axis_size("dp")
    me = lax.axis_index("dp")
    grid_rows = lax.axis_size("gr")
    bands = lax.axis_size("band")
    members = grid_rows * bands
    per_owner, _, width = left_basis.shape
    band_rows, grid_cols = gradient.shape[1], gradient.shape[2]
    piece = band_rows // grid_rows
    half = band_rows // 2
    g = gradient[0]

    def chunk(by, lo, hi):
        return lax.dynamic_slice(
            g, (lo, 0, lax.rem(me + by, n) * width), (hi - lo, grid_cols, width)
        )

    doubles = members // 4
    has_first, first_cell, second_cell, second_place, cell_slot = slot_tables(
        owner, cell, members, per_owner, doubles
    )
    from_left = shift(chunk(2, 0, half), 1, n)
    from_right = shift(chunk(2, half, band_rows), n - 1, n)
    in_left_b = shift(chunk(1, half, band_rows), 1, n)
    in_right_a = shift(chunk(n - 1, 0, half), n - 1, n)
    right_sum = added(chunk(1, 0, half), from_left)
    left_sum = added(chunk(n - 1, half, band_rows), from_right)
    in_left_a = shift(right_sum, 1, n)
    in_right_b = shift(left_sum, n - 1, n)
    summed = jnp.concatenate(
        [
            added(chunk(0, 0, half), in_left_a, in_right_a),
            added(chunk(0, half, band_rows), in_left_b, in_right_b),
        ]
    )

    right_bf = right_basis.astype(BF)
    pieces_l = [gather_columns(left_basis[s].astype(BF), n) for s in range(2)]

    spread = lax.all_to_all(
        summed.reshape(grid_rows, piece, grid_cols, width), "gr", 0, 0, tiled=True
    )
    by_cell = jnp.transpose(spread, (0, 2, 1, 3)).reshape(grid_rows * grid_cols, piece, width)
    leaving = jnp.take(by_cell, first_cell, axis=0, mode="clip")
    leaving = jnp.where((has_first > 0)[:, None, None], leaving, jnp.zeros_like(leaving))
    landed0 = lax.all_to_all(leaving, ("gr", "band"), 0, 0, tiled=True)
    pair = jnp.take(by_cell, second_cell, axis=0, mode="clip")
    pair_left = shift(pair, 1, n)
    pair_right = shift(pair, n - 1, n)
    pair_across = shift(pair, 2, n)
    pool = jnp.stack([pair, pair_left, pair_right, pair_across], axis=1)
    pool = jnp.concatenate([pool, jnp.zeros_like(pool[:1])])
    leaving = jnp.take(pool, second_place, axis=0, mode="clip")
    landed1 = lax.all_to_all(leaving, ("gr", "band"), 0, 0, tiled=True)
    pieces_g = [
        gather_columns(landed0.reshape(grid_rows, bands, piece, width), n),
        (landed1.reshape(grid_rows, bands, n, piece, width),),
    ]

    me_s = me.reshape(1).astype(jnp.int32)
    ready, late = [], ((), pieces_g[1])
    for s in range(per_owner):
        ready.append(prep(me_s, s, pieces_l[s], right_bf, first, second, late[s], n))
    state, terms = (), []
    for s in range(per_owner):
        nf, ns, own, to_right, to_left, right_t, left_b = turn(
            me_s, s, pieces_g[s], ready[s], state, n, per_owner
        )
        state = (nf, ns)
        from_left = shift(to_right, 1, n)
        from_right = shift(to_left, n - 1, n)
        top = added(right_t, from_left[: grid_rows // 2])
        bottom = added(left_b, from_right[: grid_rows // 2])
        in_left = shift(top, 1, n)
        in_right = shift(bottom, n - 1, n)
        terms.append((own, from_left, from_right, in_left, in_right))
    parted = ()
    for s in range(per_owner):
        parted = (finish(s, *terms[s], parted),)
    homed = lax.all_to_all(
        parted[0].reshape(members, per_owner, piece, width),
        ("gr", "band"), 0, 0, tiled=True,
    )
    per_cell = jnp.take(
        homed.reshape(members * per_owner, piece, width), cell_slot, axis=0, mode="clip"
    )
    final = lax.all_to_all(
        per_cell.reshape(grid_rows, grid_cols, piece, width), "gr", 0, 0, tiled=True
    )
    update = jnp.transpose(final, (0, 2, 1, 3)).reshape(band_rows, grid_cols, width)

    done = ()
    for s in range(per_owner):
        done = stats(me_s, s, pieces_g[s], left_stat, right_stat, done, n)
    return tuple(done) + state + (update,)


def solution(mesh):
    n, members = mesh.shape["dp"], mesh.shape["fsdp"]

    def run(gradient, owner, cell, *state):
        bands = state[0].shape[1] // (gradient.shape[1] // members)
        inner = Mesh(mesh.devices.reshape(n, members // bands, bands), ("dp", "gr", "band"))
        fsdp = ("gr", "band")
        part = P(fsdp, None, "dp")

        f = jax.shard_map(
            local,
            mesh=inner,
            in_specs=(P("dp", fsdp, None, None), P(), P()) + (part,) * 6,
            out_specs=(part,) * 5,
            check_vma=False,
        )
        return f(gradient, owner, cell, *state)

    return run
```

```python
import functools

import jax
import jax.numpy as jnp
from jax import lax
from jax.experimental import pallas as pl
from jax.experimental.pallas import tpu as pltpu
from jax.sharding import Mesh, PartitionSpec as P


BF = jnp.bfloat16
F32 = jnp.float32
TILE = 1024


def shift(x, by, n):
    return lax.ppermute(x, "dp", [(i, (i + by) % n) for i in range(n)])


def dot(x, y, dims):
    return lax.dot_general(x, y, (dims, ((), ())), preferred_element_type=F32)


NN = ((1,), (0,))
NT = ((1,), (1,))
TN = ((0,), (0,))


def rows_at(me, by, n, size):
    return pl.ds(pl.multiple_of(lax.rem(me + by, n) * size, size), size)


OFFSETS = (0, 3, 1, 2)


def in_vmem(x):
    return pltpu.with_memory_space_constraint(x, pltpu.MemorySpace.VMEM)


def in_hbm(x):
    return pltpu.with_memory_space_constraint(x, pltpu.MemorySpace.HBM)


def starter(sems):
    started = []

    def start(src, dst):
        c = pltpu.make_async_copy(src, dst, sems.at[len(started)])
        c.start()
        started.append(c)
        return c

    return start, started


def cols(k, width):
    return pl.ds(k * width, width)


def load_left(load, parts, lb, width):
    tall = lb.shape[0] // 2
    waits = [[load(parts[k], lb.at[:, cols(k, width)])] for k in range(3)]
    waits.append(
        [
            load(parts[3], lb.at[pl.ds(0, tall), cols(3, width)]),
            load(parts[4], lb.at[pl.ds(tall, tall), cols(3, width)]),
        ]
    )
    return waits


def load_state(load, s, me, n, r_hbm, first_hbm, second_hbm, rf, first, second):
    width = rf.shape[1]
    waits = [
        load(r_hbm.at[s, rows_at(me, OFFSETS[k], n, width), :], rf.at[cols(k, width), :])
        for k in range(4)
    ]
    return waits, [load(first_hbm.at[s], first), load(second_hbm.at[s], second)]


def prep_kernel(n, s, *refs):
    me_ref = refs[0]
    l_parts = refs[1:6]
    lb, lt, r, first, second, rf, sems = refs[-7:]
    me = me_ref[0]
    width = r.shape[1]
    load, _ = starter(sems)
    w_l = load_left(load, l_parts, lb, width)
    w_r, w_m = load_state(load, s, me, n, *refs[6:9], rf, first, second)
    for k in range(4):
        for c in w_l[k]:
            c.wait()
        lt[cols(k, width), :] = lb[:, cols(k, width)].T
    for c in w_r:
        c.wait()
    r[...] = rf[...].astype(BF)
    for c in w_m:
        c.wait()


def prep(me, s, lb, r, first, second, n):
    _, block, width = r.shape
    hbm = pl.BlockSpec(memory_space=pltpu.HBM)
    vmem = pl.BlockSpec(memory_space=pltpu.VMEM)
    return pl.pallas_call(
        functools.partial(prep_kernel, n, s),
        out_shape=[
            pltpu.VMEM((block, block), BF),
            pltpu.VMEM((block, block), BF),
            pltpu.VMEM((block, width), BF),
            pltpu.VMEM((block, width), F32),
            pltpu.VMEM((block, width), F32),
        ],
        in_specs=[pl.BlockSpec(memory_space=pltpu.SMEM)] + [hbm] * 8,
        out_specs=[vmem] * 5,
        scratch_shapes=[pltpu.VMEM((block, width), F32), pltpu.SemaphoreType.DMA((11,))],
        compiler_params=pltpu.CompilerParams(vmem_limit_bytes=20 * 2**20),
        cost_estimate=pl.CostEstimate(flops=2**22, bytes_accessed=6 * 2**20, transcendentals=0),
        name="prep",
    )(me, *[in_hbm(x) for x in (*lb, r, first, second)])


def flip_kernel(*refs):
    l_parts, out = refs[:5], refs[5]
    lb, lt, sems, out_sems = refs[6:]
    width = l_parts[0].shape[1]
    load, _ = starter(sems)
    store, stores = starter(out_sems)
    w_l = load_left(load, l_parts, lb, width)
    for k in range(4):
        for c in w_l[k]:
            c.wait()
        lt[cols(k, width), :] = lb[:, cols(k, width)].T
        store(lt.at[cols(k, width), :], out.at[cols(k, width), :])
    for c in stores:
        c.wait()


def flip(lb):
    block = lb[0].shape[0]
    hbm = pl.BlockSpec(memory_space=pltpu.HBM)
    return pl.pallas_call(
        flip_kernel,
        out_shape=pltpu.HBM((block, block), BF),
        in_specs=[hbm] * 5,
        out_specs=hbm,
        scratch_shapes=[
            pltpu.VMEM((block, block), BF),
            pltpu.VMEM((block, block), BF),
            pltpu.SemaphoreType.DMA((5,)),
            pltpu.SemaphoreType.DMA((4,)),
        ],
        compiler_params=pltpu.CompilerParams(vmem_limit_bytes=20 * 2**20),
        cost_estimate=pl.CostEstimate(flops=2**22, bytes_accessed=4 * 2**20, transcendentals=0),
        name="flip",
    )(*[in_hbm(x) for x in lb])


def load_grad(load, s, parts, g, width, near=False):
    pieces = g.shape[1]
    half = pieces // 2
    waits = []
    if s == 0:
        for k, ref in enumerate(parts[:3]):
            waits += [load(ref.at[q], g.at[:, q, :, cols(k, width)]) for q in range(pieces)]
        for q in range(half):
            if near:
                g[:, q, :, 3 * width :] = parts[3][q]
                g[:, q + half, :, 3 * width :] = parts[4][q]
            else:
                waits.append(load(parts[3].at[q], g.at[:, q, :, cols(3, width)]))
                waits.append(load(parts[4].at[q], g.at[:, q + half, :, cols(3, width)]))
    elif near:
        for k in range(4):
            for q in range(pieces):
                g[:, q, :, k * width : (k + 1) * width] = parts[0][q, :, k]
    else:
        for k in range(4):
            waits += [
                load(parts[0].at[q, :, k], g.at[:, q, :, cols(k, width)]) for q in range(pieces)
            ]
    return waits


def turn_kernel(n, s, count, *refs):
    me_ref = refs[0]
    g_parts = refs[1 : 1 + count]
    if s == 0:
        lb, lt, r, first, second = refs[1 + count : 6 + count]
    else:
        l_parts = refs[1 + count : 6 + count]
        lt_hbm = refs[6 + count]
        hold = refs[7 + count : 10 + count]
        lb, lt, r, first, second, rf, own_sems = refs[-16:-9]
        refs = refs[:-16] + refs[-9:]
    nf_hbm, ns_hbm, own_out, to_right, to_left, right_t, left_b = refs[-16:-9]
    g, z, d, t, p, nf, ns, sems, out_sems = refs[-9:]
    me = me_ref[0]
    _, pieces, piece, block = g.shape
    width = z.shape[1]
    half = pieces // 2
    load, _ = starter(sems)
    store, stores = starter(out_sems)
    w_r, w_t, w_m, w_l = [], [], [], []
    if s == 1:
        fetch, _ = starter(own_sems)
        w_r, w_m = load_state(fetch, s, me, n, *hold, rf, first, second)
        w_t = [fetch(lt_hbm, lt)]
        w_l = load_left(fetch, l_parts, lb, width)
    for c in load_grad(load, s, g_parts, g, width, near=True):
        c.wait()
    for c in w_r:
        c.wait()
    if s == 1:
        r[...] = rf[...].astype(BF)
    per = TILE // (pieces * piece)
    tiles = block // TILE

    @pl.loop(0, tiles)
    def _(i):
        rows = g[pl.ds(i * per, per)].reshape(TILE, block)
        at = pl.ds(pl.multiple_of(i * TILE, TILE), TILE)
        z[at, :] = dot(rows, r[...], NN).astype(BF)

    for c in w_t + w_m:
        c.wait()
    for k in range(4):
        at = rows_at(me, OFFSETS[k], n, width)
        turned = dot(lt[cols(k, width), :], z[...], NN)
        a = 0.9 * first[at, :] + 0.1 * turned
        b = 0.999 * second[at, :] + 0.001 * turned * turned
        nf[at, :] = a
        ns[at, :] = b
        d[cols(k, width), :] = (a / (jnp.sqrt(b) + 1e-8)).astype(BF)
    store(nf, nf_hbm.at[s])
    store(ns, ns_hbm.at[s])
    for group in w_l:
        for c in group:
            c.wait()

    @pl.loop(0, tiles)
    def _(i):
        at = pl.ds(pl.multiple_of(i * TILE, TILE), TILE)
        t[at, :] = dot(lb[at, :], d[...], NN).astype(BF)

    for k in (3, 2, 1, 0):

        @pl.loop(0, tiles)
        def _(i):
            at = pl.ds(pl.multiple_of(i * TILE, TILE), TILE)
            v = dot(t[at, :], r[cols(k, width), :], NT).astype(BF)
            p[pl.ds(i * per, per), :, :, cols(k, width)] = v.reshape(per, pieces, piece, width)

        for q in range(pieces):
            src = p.at[:, q, :, cols(k, width)]
            low = q < half
            if k == 0:
                store(src, own_out.at[q])
            elif k == 3:
                store(src, to_right.at[q] if low else to_left.at[q - half])
            elif k == 2:
                store(src, right_t.at[q] if low else to_right.at[q])
            else:
                store(src, to_left.at[q + half] if low else left_b.at[q - half])
    for c in stores:
        c.wait()


def turn(me, s, g, ready, before, n, per_owner):
    block, width = ready[0].shape[0], g[0].shape[-1]
    pieces, bands, piece = g[0].shape[0], g[0].shape[1], g[0].shape[-2]
    hbm = pl.BlockSpec(memory_space=pltpu.HBM)
    vmem = pl.BlockSpec(memory_space=pltpu.VMEM)
    far = 3 if s == 0 else 0
    extra = []
    if s == 1:
        extra = [pltpu.VMEM((block, block), BF)] * 2 + [pltpu.VMEM((block, width), BF)]
        extra += [pltpu.VMEM((block, width), F32)] * 3 + [pltpu.SemaphoreType.DMA((12,))]
    state = pltpu.HBM((per_owner, block, width), F32)
    whole = pltpu.HBM((pieces, bands, piece, width), BF)
    part = pltpu.HBM((pieces // 2, bands, piece, width), BF)
    return pl.pallas_call(
        functools.partial(turn_kernel, n, s, len(g)),
        out_shape=[state, state, whole, whole, whole, part, part],
        in_specs=[pl.BlockSpec(memory_space=pltpu.SMEM)]
        + [hbm] * far
        + [vmem] * (len(g) - far)
        + [vmem if s == 0 else hbm] * len(ready)
        + [hbm] * len(before),
        out_specs=[hbm] * 7,
        scratch_shapes=extra
        + [
            pltpu.VMEM((bands, pieces, piece, block), BF),
            pltpu.VMEM((block, width), BF),
            pltpu.VMEM((block, width), BF),
            pltpu.VMEM((block, width), BF),
            pltpu.VMEM((bands, pieces, piece, block), BF),
            pltpu.VMEM((block, width), F32),
            pltpu.VMEM((block, width), F32),
            pltpu.SemaphoreType.DMA((16,)),
            pltpu.SemaphoreType.DMA((18,)),
        ],
        input_output_aliases={1 + len(ready) + len(g) + i: i for i in range(len(before))},
        compiler_params=pltpu.CompilerParams(vmem_limit_bytes=(20 if s == 0 else 32) * 2**20),
        cost_estimate=pl.CostEstimate(
            flops=8 * block * block * width, bytes_accessed=6 * 2**20, transcendentals=0
        ),
        name="turn",
    )(
        me,
        *[in_hbm(x) for x in g[:far]],
        *[in_vmem(x) for x in g[far:]],
        *[in_vmem(x) if s == 0 else in_hbm(x) for x in ready],
        *[in_hbm(x) for x in before],
    )


def stats_kernel(n, s, count, *refs):
    me_ref = refs[0]
    g_parts = refs[1 : 1 + count]
    lstat, rstat = refs[1 + count : 3 + count]
    new_l, new_r, g, sems = refs[-4:]
    me = me_ref[0]
    _, _, _, block = g.shape
    width = lstat.shape[2]
    load, _ = starter(sems)
    for c in load_grad(load, s, g_parts, g, width):
        c.wait()
    flat = g.reshape(block, block)

    @pl.loop(0, block // TILE)
    def _(i):
        at = pl.ds(pl.multiple_of(i * TILE, TILE), TILE)
        acc = dot(flat[at, :], flat[rows_at(me, 0, n, width), :], NT)
        new_l[0, at, :] = 0.95 * lstat[0, at, :] + 0.05 * acc

    for k in range(4):
        at = rows_at(me, OFFSETS[k], n, width)
        acc = dot(flat[:, cols(k, width)], flat[:, cols(0, width)], TN)
        new_r[0, at, :] = 0.95 * rstat[0, at, :] + 0.05 * acc


def stats(me, s, g, lstat, rstat, before, n):
    _, block, width = lstat.shape
    pieces, bands, piece = g[0].shape[0], g[0].shape[1], g[0].shape[-2]
    slot = pl.BlockSpec((1, block, width), lambda i: (s, 0, 0))
    hbm = pl.BlockSpec(memory_space=pltpu.HBM)
    out = jax.ShapeDtypeStruct(lstat.shape, F32)
    return pl.pallas_call(
        functools.partial(stats_kernel, n, s, len(g)),
        grid=(1,),
        out_shape=[out, out],
        in_specs=[pl.BlockSpec(memory_space=pltpu.SMEM)]
        + [hbm] * len(g)
        + [slot, slot]
        + [hbm] * len(before),
        out_specs=[slot, slot],
        scratch_shapes=[
            pltpu.VMEM((bands, pieces, piece, block), BF),
            pltpu.SemaphoreType.DMA((16,)),
        ],
        input_output_aliases={3 + len(g) + i: i for i in range(len(before))},
        compiler_params=pltpu.CompilerParams(vmem_limit_bytes=24 * 2**20),
        cost_estimate=pl.CostEstimate(
            flops=4 * block * block * width, bytes_accessed=6 * 2**20, transcendentals=0
        ),
        name="stats",
    )(me, *[in_hbm(x) for x in g], lstat, rstat, *before)


def finish_kernel(s, *refs):
    own, from_left, from_right, in_left, in_right = refs[:5]
    out, a, b, sems, out_sems = refs[-5:]
    pieces = own.shape[0]
    half = pieces // 2
    load, loads = starter(sems)
    load(own, a)
    load(from_right.at[pl.ds(half, half)], b.at[pl.ds(0, half)])
    load(from_left.at[pl.ds(half, half)], b.at[pl.ds(half, half)])
    for x in loads:
        x.wait()
    store, stores = starter(out_sems)
    for q in range(pieces):
        c = in_left[q] if q < half else in_right[q - half]
        a[q] = (a[q].astype(F32) + b[q].astype(F32) + c.astype(F32)).astype(BF)
        store(a.at[q], out.at[q, :, s])
    for x in stores:
        x.wait()


def finish(s, own, from_left, from_right, in_left, in_right, before):
    pieces, bands, piece, width = own.shape
    hbm = pl.BlockSpec(memory_space=pltpu.HBM)
    vmem = pl.BlockSpec(memory_space=pltpu.VMEM)
    return pl.pallas_call(
        functools.partial(finish_kernel, s),
        out_shape=pltpu.HBM((pieces, bands, 2, piece, width), BF),
        in_specs=[hbm] * 3 + [vmem] * 2 + [hbm] * len(before),
        out_specs=hbm,
        scratch_shapes=[pltpu.VMEM(own.shape, BF)] * 2
        + [pltpu.SemaphoreType.DMA((3,)), pltpu.SemaphoreType.DMA((pieces,))],
        input_output_aliases={5 + i: i for i in range(len(before))},
        compiler_params=pltpu.CompilerParams(vmem_limit_bytes=16 * 2**20),
        cost_estimate=pl.CostEstimate(flops=2**20, bytes_accessed=2 * 2**20, transcendentals=0),
        name="finish",
    )(
        *[in_hbm(x) for x in (own, from_left, from_right)],
        in_vmem(in_left),
        in_vmem(in_right),
        *[in_hbm(x) for x in before],
    )


def gather_columns(x, n):
    half = x.shape[0] // 2
    left = shift(x, 1, n)
    right = shift(x, n - 1, n)
    top = shift(left[:half], 1, n)
    bottom = shift(right[half:], n - 1, n)
    return x, left, right, top, bottom


def slot_tables(owner, cell, members, per_owner, doubles):
    ids = jnp.arange(owner.shape[0], dtype=jnp.int32)
    shared = (owner[:, None] == owner[None, :]) & (ids[None, :] < ids[:, None])
    rank = jnp.sum(shared.astype(jnp.int32), axis=1)
    cells = jnp.arange(owner.shape[0], dtype=jnp.int32)
    hit = (cell[None, :] == cells[:, None]).astype(jnp.int32)
    cell_slot = jnp.sum(hit * (owner * per_owner + rank)[None, :], axis=1)
    who = jnp.arange(members, dtype=jnp.int32)
    mine = owner[None, :] == who[:, None]
    first = (mine & (rank == 0)[None, :]).astype(jnp.int32)
    second = (mine & (rank == 1)[None, :]).astype(jnp.int32)
    has_first = jnp.sum(first, axis=1)
    first_cell = jnp.sum(first * cell[None, :], axis=1)
    is_second = rank == 1
    before = jnp.sum((is_second[None, :] & (ids[None, :] < ids[:, None])).astype(jnp.int32), axis=1)
    place = jnp.where(is_second, before, doubles)
    second_place = jnp.sum(second * (place - doubles)[None, :], axis=1) + doubles
    spots = jnp.arange(doubles, dtype=jnp.int32)
    second_cell = jnp.sum((place[None, :] == spots[:, None]).astype(jnp.int32) * cell[None, :], axis=1)
    return has_first, first_cell, second_cell, second_place, cell_slot


def added(*xs):
    return sum(x.astype(F32) for x in xs).astype(BF)


def local(gradient, owner, cell, left_basis, right_basis, left_stat, right_stat, first, second):
    n = lax.axis_size("dp")
    me = lax.axis_index("dp")
    grid_rows = lax.axis_size("gr")
    bands = lax.axis_size("band")
    members = grid_rows * bands
    per_owner, _, width = left_basis.shape
    band_rows, grid_cols = gradient.shape[1], gradient.shape[2]
    piece = band_rows // grid_rows
    half = band_rows // 2
    g = gradient[0]

    def chunk(by, lo, hi):
        return lax.dynamic_slice(
            g, (lo, 0, lax.rem(me + by, n) * width), (hi - lo, grid_cols, width)
        )

    doubles = members // 4
    has_first, first_cell, second_cell, second_place, cell_slot = slot_tables(
        owner, cell, members, per_owner, doubles
    )
    from_left = shift(chunk(2, 0, half), 1, n)
    from_right = shift(chunk(2, half, band_rows), n - 1, n)
    in_left_b = shift(chunk(1, half, band_rows), 1, n)
    in_right_a = shift(chunk(n - 1, 0, half), n - 1, n)
    right_sum = added(chunk(1, 0, half), from_left)
    left_sum = added(chunk(n - 1, half, band_rows), from_right)
    in_left_a = shift(right_sum, 1, n)
    in_right_b = shift(left_sum, n - 1, n)
    summed = jnp.concatenate(
        [
            added(chunk(0, 0, half), in_left_a, in_right_a),
            added(chunk(0, half, band_rows), in_left_b, in_right_b),
        ]
    )

    pieces_l = [gather_columns(left_basis[s].astype(BF), n) for s in range(2)]

    spread = lax.all_to_all(
        summed.reshape(grid_rows, piece, grid_cols, width), "gr", 0, 0, tiled=True
    )
    by_cell = jnp.transpose(spread, (0, 2, 1, 3)).reshape(grid_rows * grid_cols, piece, width)
    leaving = jnp.take(by_cell, first_cell, axis=0, mode="clip")
    leaving = jnp.where((has_first > 0)[:, None, None], leaving, jnp.zeros_like(leaving))
    landed0 = lax.all_to_all(leaving, ("gr", "band"), 0, 0, tiled=True)
    pair = jnp.take(by_cell, second_cell, axis=0, mode="clip")
    pair_left = shift(pair, 1, n)
    pair_right = shift(pair, n - 1, n)
    pair_across = shift(pair, 2, n)
    pool = jnp.stack([pair, pair_left, pair_right, pair_across], axis=1)
    pool = jnp.concatenate([pool, jnp.zeros_like(pool[:1])])
    leaving = jnp.take(pool, second_place, axis=0, mode="clip")
    landed1 = lax.all_to_all(leaving, ("gr", "band"), 0, 0, tiled=True)
    pieces_g = [
        gather_columns(landed0.reshape(grid_rows, bands, piece, width), n),
        (landed1.reshape(grid_rows, bands, n, piece, width),),
    ]

    me_s = me.reshape(1).astype(jnp.int32)
    held = prep(me_s, 0, pieces_l[0], right_basis, first, second, n)
    flipped = flip(pieces_l[1])
    ready = [held, (*pieces_l[1], flipped, right_basis, first, second)]
    state, terms = (), []
    for s in range(per_owner):
        nf, ns, own, to_right, to_left, right_t, left_b = turn(
            me_s, s, pieces_g[s], ready[s], state, n, per_owner
        )
        state = (nf, ns)
        from_left = shift(to_right, 1, n)
        from_right = shift(to_left, n - 1, n)
        top = added(right_t, from_left[: grid_rows // 2])
        bottom = added(left_b, from_right[: grid_rows // 2])
        in_left = shift(top, 1, n)
        in_right = shift(bottom, n - 1, n)
        terms.append((own, from_left, from_right, in_left, in_right))
    parted = ()
    for s in range(per_owner):
        parted = (finish(s, *terms[s], parted),)
    homed = lax.all_to_all(
        parted[0].reshape(members, per_owner, piece, width),
        ("gr", "band"), 0, 0, tiled=True,
    )
    per_cell = jnp.take(
        homed.reshape(members * per_owner, piece, width), cell_slot, axis=0, mode="clip"
    )
    final = lax.all_to_all(
        per_cell.reshape(grid_rows, grid_cols, piece, width), "gr", 0, 0, tiled=True
    )
    update = jnp.transpose(final, (0, 2, 1, 3)).reshape(band_rows, grid_cols, width)

    done = ()
    for s in range(per_owner):
        done = stats(me_s, s, pieces_g[s], left_stat, right_stat, done, n)
    return tuple(done) + state + (update,)


def solution(mesh):
    n, members = mesh.shape["dp"], mesh.shape["fsdp"]

    def run(gradient, owner, cell, *state):
        bands = state[0].shape[1] // (gradient.shape[1] // members)
        inner = Mesh(mesh.devices.reshape(n, members // bands, bands), ("dp", "gr", "band"))
        fsdp = ("gr", "band")
        part = P(fsdp, None, "dp")

        f = jax.shard_map(
            local,
            mesh=inner,
            in_specs=(P("dp", fsdp, None, None), P(), P()) + (part,) * 6,
            out_specs=(part,) * 5,
            check_vma=False,
        )
        return f(gradient, owner, cell, *state)

    return run
```
